32 devices in a mesh: sky: 2 (over y), ma: 4 (over z), freq: 2 (over x), pol: 2 (over core).
Axes of the slice: x: 2, y: 2, z: 4, core: 2. Of those that a mesh axis runs over, the one named last changes fastest.
Arguments:
- alm: bfloat16 [2, 2, 1024, 4, 1024], P(None, 'freq', ('ma', 'pol'), None, 'sky'), parts along dimension 4, may hold values from -6 to 6
- beam: bfloat16 [4, 2, 2, 1024, 1024], P('ma', 'freq', None, 'pol'), may hold values from -0.1875 to 0.1875
- m_table: int32 [4], P('ma'), may hold values from 0 to 511, as said below
- chan_mask: int32 [2], P('freq'), may hold values from 0 to 1, as said below
- noise: float32 [2, 1024], P('freq', 'pol'), may hold values from 0.5 to 4
Outputs:
- scaled: bfloat16 [2, 2, 4, 1024, 1024], P(None, 'freq', 'ma', 'pol', 'sky'), parts along dimension 4
- channel_power: float32 [4], P(('sky', 'freq')), parts along dimension 0
The draws below stay inside these ranges and needn't reach their ends.
There are 2 independent parts, one for each index of `sky`. The reference program is written for one: setup_inputs(seed, part) draws one part's arguments, and reference() takes and returns one part's arrays. A program takes and returns all parts, laid end to end along the dimension named above; an argument that names none is the same for every part. Nothing has to cross between parts.
Inputs may be any that keep to these rules, and one draw needn't show every extreme that they name: `m_table`: the 4 values are distinct whole numbers below 512. `chan_mask`: at least one of the 2 channels is usable.
All inputs are finite; a program needn't handle non-finite values.
Results may differ from the reference program's by a relative error of at most 0.00055.
Values may be sent and summed in bfloat16 or wider, within the bound.
A program may use at most 64 MiB of HBM per device.

```python
import math
import jax
import jax.numpy as jnp
from jax import lax

L = 1024
K = 1024
S = 512
M = 4
F = 2


def draw_m_table(key, part):
    return jax.random.permutation(key, L // 2)[:M].astype(jnp.int32)


def draw_chan_mask(key, part):
    mask_key = jax.random.fold_in(key, 23)
    first_key, second_key = jax.random.split(mask_key)
    flags = (jax.random.randint(first_key, (F,), 0, 4) < 3).astype(jnp.int32)
    chosen = jax.random.randint(second_key, (), 0, F)
    forced = (jnp.arange(F, dtype=jnp.int32) == chosen).astype(jnp.int32)
    return jnp.maximum(flags, forced).astype(jnp.int32)


def block_scale(stream_key, shape, pieces, least, top_value):
    loudness, own = 1.0, jax.random.fold_in(stream_key, 6)
    for dim, parts in pieces:
        draws = jnp.exp(jax.random.uniform(jax.random.fold_in(own, dim), (parts,), jnp.float32, least / len(pieces), top_value / len(pieces)))
        loudness = loudness * jnp.repeat(draws, shape[dim] // parts).reshape([-1 if axis == dim else 1 for axis in range(len(shape))])
    return loudness


def scatter_about(rng, dims, spread, reach, shards=(), held_as=jnp.bfloat16):
    result = spread * jax.random.normal(rng, dims, jnp.float32)
    if shards:
        result = result * block_scale(rng, dims, shards, -0.22, 0.18)
    return jnp.clip(result, -reach, reach).astype(held_as)


def setup_inputs(seed: int = 0, part: int = 0) -> dict:
    key_of = jax.random.split(jax.random.key(seed), 6)
    part_keys = jax.random.split(jax.random.fold_in(key_of[5], part), 6)
    return {
        "alm": scatter_about(part_keys[0], (2, F, L, M, S), 1.0, 6.0, ((1, 2), (2, 8))),
        "beam": scatter_about(key_of[1], (M, F, 2, K, L), L ** -0.5, 0.1875, ((0, 4), (1, 2), (3, 2))),
        "m_table": draw_m_table(jax.random.fold_in(key_of[5], 71), part),
        "chan_mask": draw_chan_mask(jax.random.fold_in(key_of[5], 71), part),
        "noise": jnp.clip(jnp.exp(math.log(4.0) - 2.0794415 * jax.random.uniform(key_of[4], (F, K), jnp.float32) ** block_scale(key_of[4], (F, K), ((0, 2), (1, 2)), -0.2, 0.2)), 0.5, 4.0),
    }


def reference(alm, beam, m_table, chan_mask, noise):
    degree = jnp.arange(L, dtype=jnp.int32)

    def one_mode(inputs):
        response, coeffs, m_value = inputs
        keep_mask = (degree >= m_value)[None, None, :, None]
        active = jnp.where(keep_mask, coeffs, jnp.zeros((), coeffs.dtype)).astype(jnp.float32)
        response = response.astype(jnp.float32)
        real_part = jnp.einsum('fkl,fls->fks', response[:, 0], active[0]) - jnp.einsum('fkl,fls->fks', response[:, 1], active[1])
        imag_part = jnp.einsum('fkl,fls->fks', response[:, 0], active[1]) + jnp.einsum('fkl,fls->fks', response[:, 1], active[0])
        return jnp.stack([real_part, imag_part])
    per_mode = lax.map(one_mode, (beam, jnp.moveaxis(alm, 3, 0), m_table))
    visibility = jnp.transpose(per_mode, (1, 2, 0, 3, 4))
    weighted = visibility * visibility / noise[None, :, None, :, None]
    channel_power = lax.optimization_barrier(jnp.sum(weighted, axis=(0, 2, 3, 4))) / jnp.float32(M * K * S)
    mask_float = chan_mask.astype(jnp.float32)
    live_count = jnp.sum(mask_float)
    band_power = jnp.sum(mask_float * channel_power) / live_count
    factor = mask_float / jnp.sqrt(0.5 * channel_power + 0.5 * band_power + 1e-06)
    scaled = visibility * (lax.rsqrt(noise) * factor[:, None])[None, :, None, :, None]
    return (scaled.astype(jnp.bfloat16), channel_power)
```

```python
import functools

import jax
import jax.numpy as jnp
from jax import lax
from jax.experimental import pallas as pl
from jax.experimental.pallas import tpu as pltpu
from jax.sharding import PartitionSpec as P

MESH = pl.DeviceIdType.MESH


def near_first(n, me):
    if n > 8:
        shifts = [s for k in range(1, n // 2 + 1) for s in (k, n - k)][: n - 1]
        return [lax.rem(me + s, n) for s in shifts]
    table = [sorted((j for j in range(n) if j != i), key=lambda j: (abs(j - i), j)) for i in range(n)]
    order = []
    for k in range(n - 1):
        pick = jnp.int32(table[0][k])
        for i in range(1, n):
            pick = jnp.where(me == i, jnp.int32(table[i][k]), pick)
        order.append(pick)
    return order


def step_kernel(
    sizes, total, alm_ref, beam_ref, m_ref, mask_ref, noise_ref, out_ref, power_ref,
    recv, wide, acc, beam_v, inv_n, rs_n, mine, slots,
    z_send, z_recv, p_send, p_recv, own_sem, beam_sem, q_send, q_recv,
):
    n_ma, n_freq, n_pol = sizes
    n_all = n_ma * n_freq * n_pol
    ma, freq, pol = lax.axis_index("ma"), lax.axis_index("freq"), lax.axis_index("pol")
    block, columns = alm_ref.shape[2], alm_ref.shape[3]
    groups, _, rows, _ = recv.shape
    per_source = n_pol * block
    per_group = rows // per_source
    modes = beam_ref.shape[1]
    my_slot = (freq * n_ma + ma) * n_pol + pol

    def place(slot):
        return {"ma": lax.rem(slot // n_pol, n_ma), "freq": slot // (n_pol * n_ma), "pol": lax.rem(slot, n_pol)}

    def for_peers(body):
        if n_all <= 32:
            for r in range(1, n_all):
                body(r)
        else:
            lax.fori_loop(1, n_all, lambda r, _: (body(r), 0)[1], 0)

    beam_copy = pltpu.make_async_copy(beam_ref, beam_v, beam_sem)
    beam_copy.start()

    barrier = pltpu.get_barrier_semaphore()

    def greet(r):
        pl.semaphore_signal(barrier, inc=1, device_id=place(lax.rem(my_slot + r, n_all)), device_id_type=MESH)

    for_peers(greet)

    def part(source, core, c):
        start = lax.rem(source, per_group) * per_source + core * block
        return recv.at[source // per_group, c, pl.ds(pl.multiple_of(start, block), block)]

    own = [pltpu.make_async_copy(alm_ref.at[ma, c], part(ma, pol, c), own_sem.at[c]) for c in range(2)]
    for copy in own:
        copy.start()
    pl.semaphore_wait(barrier, n_all - 1)

    order = near_first(n_ma, ma)
    sends = []
    for k, dest in enumerate(order):
        for c in range(2):
            sends.append(pltpu.make_async_remote_copy(
                src_ref=alm_ref.at[dest, c], dst_ref=part(ma, pol, c),
                send_sem=z_send.at[k, c], recv_sem=z_recv.at[ma, c],
                device_id={"ma": dest}, device_id_type=MESH))
            sends[-1].start()

    def relay(source, c, src):
        hops = []
        for q in range(1, n_pol):
            hops.append(pltpu.make_async_remote_copy(
                src_ref=src, dst_ref=part(source, pol, c),
                send_sem=p_send.at[source, c], recv_sem=p_recv.at[source, c],
                device_id={"pol": lax.rem(pol + q, n_pol)}, device_id_type=MESH))
            hops[-1].start()
        return hops

    def arrival(source, c):
        return pltpu.make_async_remote_copy(
            src_ref=alm_ref.at[source, c], dst_ref=part(source, pol, c),
            send_sem=z_send.at[0, c], recv_sem=z_recv.at[source, c],
            device_id={"ma": source}, device_id_type=MESH)

    relays = [relay(ma, c, alm_ref.at[ma, c]) for c in range(2)]

    spread = jnp.transpose(jnp.broadcast_to(noise_ref[...], (128, modes)))
    inv_n[...] = 1.0 / spread
    rs_n[...] = lax.rsqrt(spread)
    mine[1:2, :] = jnp.full((1, 128), mask_ref[0].astype(jnp.float32))
    beam_copy.wait()
    strip = min(modes, 128)

    def widen(i, _):
        k0 = pl.multiple_of(i * strip, strip)
        for g in range(groups):
            degree = lax.broadcasted_iota(jnp.int32, (strip, rows), 1) + g * rows
            keep = degree >= m_ref[0]
            zero = jnp.zeros((strip, rows), jnp.float32)
            b0 = jnp.where(keep, beam_v[0, pl.ds(k0, strip), g * rows:(g + 1) * rows].astype(jnp.float32), zero)
            b1 = jnp.where(keep, beam_v[1, pl.ds(k0, strip), g * rows:(g + 1) * rows].astype(jnp.float32), zero)
            wide[g, 0, pl.ds(k0, strip), :] = b0.astype(wide.dtype)
            wide[g, 1, pl.ds(k0, strip), :] = (-b1).astype(wide.dtype)
            wide[g, 0, pl.ds(modes + k0, strip), :] = b1.astype(wide.dtype)
            wide[g, 1, pl.ds(modes + k0, strip), :] = b0.astype(wide.dtype)
        return 0

    lax.fori_loop(0, modes // strip, widen, 0)

    tile = min(modes, 256)
    tiles = 2 * modes // tile

    def accumulate(g, first):
        def body(i, _):
            k0 = pl.multiple_of(i * tile, tile)
            value = jnp.dot(wide[g, 0, pl.ds(k0, tile), :], recv[g, 0], preferred_element_type=jnp.float32)
            value += jnp.dot(wide[g, 1, pl.ds(k0, tile), :], recv[g, 1], preferred_element_type=jnp.float32)
            acc[pl.ds(k0, tile), :] = value if first else acc[pl.ds(k0, tile), :] + value
            return 0
        lax.fori_loop(0, tiles, body, 0)

    def squares(value, k0):
        noise_rows = inv_n[pl.ds(lax.rem(k0, modes), tile), :]
        sums = jnp.zeros((tile, 128), jnp.float32)
        for j in range(columns // 128):
            part_j = value[:, j * 128:(j + 1) * 128]
            sums += part_j * part_j
        return jnp.sum(sums * noise_rows, axis=0, keepdims=True)

    def finish(steps):
        def body(i, power):
            k0 = pl.multiple_of(i * tile, tile)
            value = acc[pl.ds(k0, tile), :]
            for g, c in steps:
                value += jnp.dot(wide[g, c, pl.ds(k0, tile), :], recv[g, c], preferred_element_type=jnp.float32)
            acc[pl.ds(k0, tile), :] = value
            return power + squares(value, k0)
        return lax.fori_loop(0, tiles, body, jnp.zeros((1, 128), jnp.float32))

    def add_half(g, c):
        def body(i, _):
            k0 = pl.multiple_of(i * tile, tile)
            acc[pl.ds(k0, tile), :] += jnp.dot(wide[g, c, pl.ds(k0, tile), :], recv[g, c], preferred_element_type=jnp.float32)
            return 0
        lax.fori_loop(0, tiles, body, 0)

    for copy in own:
        copy.wait()
    for c in range(2):
        for hop in relays[c]:
            hop.wait()
    if per_group == 1:
        accumulate(ma, True)
        for k, source in enumerate(order):
            later = []
            for c in range(2):
                arrival(source, c).wait_recv()
                later.append(relay(source, c, part(source, pol, c)))
            if k < len(order) - 1:
                for c in range(2):
                    for hop in later[c]:
                        hop.wait()
                accumulate(source, False)
            else:
                for hop in later[0]:
                    hop.wait()
                add_half(source, 0)
                for hop in later[1]:
                    hop.wait()
                power = finish([(source, 1)])
    else:
        later = []
        for source in order:
            for c in range(2):
                arrival(source, c).wait_recv()
                later.append(relay(source, c, part(source, pol, c)))
        for hops in later:
            for hop in hops:
                hop.wait()
        for g in range(groups):
            accumulate(g, g == 0)
        power = finish([])

    mine[0:1, :] = power
    slots[my_slot, 0:1, :] = power
    slots[my_slot, 1:2, :] = mine[1:2, :]

    def report(r):
        return pltpu.make_async_remote_copy(
            src_ref=mine, dst_ref=slots.at[my_slot], send_sem=q_send.at[r - 1], recv_sem=q_recv.at[my_slot],
            device_id=place(lax.rem(my_slot + r, n_all)), device_id_type=MESH)

    def heard(r):
        source = lax.rem(my_slot + r, n_all)
        pltpu.make_async_remote_copy(
            src_ref=mine, dst_ref=slots.at[source], send_sem=q_send.at[r - 1], recv_sem=q_recv.at[source],
            device_id=place(source), device_id_type=MESH).wait_recv()

    for_peers(lambda r: report(r).start())
    for copy in sends:
        copy.wait_send()
    for_peers(heard)

    per_freq = n_ma * n_pol
    masked, live, here = 0.0, 0.0, 0.0
    for f in range(n_freq):
        channel = jnp.sum(jnp.sum(slots[f * per_freq:(f + 1) * per_freq, 0, :], axis=0, keepdims=True), axis=1, keepdims=True) / total
        flag = slots[f * per_freq, 1:2, 0:1]
        masked += flag * channel
        live += flag
        here += jnp.where(freq == f, channel, 0.0)
    band = masked / live
    factor = mine[1:2, 0:1] / jnp.sqrt(0.5 * here + 0.5 * band + 1e-06)
    power_ref[0] = here[0, 0]

    def rescale(i, _):
        k0 = pl.multiple_of(i * strip, strip)
        scale = rs_n[pl.ds(k0, strip), :] * factor
        for c in range(2):
            for j in range(columns // 128):
                value = acc[pl.ds(c * modes + k0, strip), j * 128:(j + 1) * 128]
                out_ref[c, pl.ds(k0, strip), j * 128:(j + 1) * 128] = (value * scale).astype(out_ref.dtype)
        return 0

    lax.fori_loop(0, modes // strip, rescale, 0)
    for_peers(lambda r: report(r).wait_send())


def on_device(sizes, alm, beam, m_table, chan_mask, noise):
    n_ma, n_freq, n_pol = sizes
    planes = jnp.transpose(alm[:, 0], (2, 0, 1, 3))
    response = beam[0, 0]
    block, columns = planes.shape[2], planes.shape[3]
    modes, degrees = response.shape[1], response.shape[2]
    per_source = n_pol * block
    rows = per_source * max(1, min(n_ma, 256 // per_source))
    groups = degrees // rows
    n_all = n_ma * n_freq * n_pol
    total = float(n_ma * modes * n_pol * columns)
    vmem = pl.BlockSpec(memory_space=pltpu.VMEM)
    smem = pl.BlockSpec(memory_space=pltpu.SMEM)
    dma = pltpu.SemaphoreType.DMA
    scaled, power = pl.pallas_call(
        functools.partial(step_kernel, sizes, total),
        out_shape=(
            jax.ShapeDtypeStruct((2, modes, columns), jnp.bfloat16),
            jax.ShapeDtypeStruct((1,), jnp.float32),
        ),
        in_specs=[vmem, pl.BlockSpec(memory_space=pl.ANY), smem, smem, vmem],
        out_specs=(vmem, smem),
        scratch_shapes=[
            pltpu.VMEM((groups, 2, rows, columns), jnp.bfloat16),
            pltpu.VMEM((groups, 2, 2 * modes, rows), jnp.bfloat16),
            pltpu.VMEM((2 * modes, columns), jnp.float32),
            pltpu.VMEM((2, modes, degrees), jnp.bfloat16),
            pltpu.VMEM((modes, 128), jnp.float32),
            pltpu.VMEM((modes, 128), jnp.float32),
            pltpu.VMEM((2, 128), jnp.float32),
            pltpu.VMEM((n_all, 2, 128), jnp.float32),
            dma((n_ma, 2)), dma((n_ma, 2)), dma((n_ma, 2)), dma((n_ma, 2)), dma((2,)), dma,
            dma((n_all,)), dma((n_all,)),
        ],
        compiler_params=pltpu.CompilerParams(collective_id=0, has_side_effects=True, vmem_limit_bytes=40 * 1024 * 1024),
        name="driftscan_step",
    )(planes, response, m_table, chan_mask, noise)
    return scaled[:, None, None], power


def solution(mesh):
    sizes = (mesh.shape["ma"], mesh.shape["freq"], mesh.shape["pol"])
    return jax.shard_map(
        functools.partial(on_device, sizes),
        mesh=mesh,
        in_specs=(
            P(None, "freq", ("ma", "pol"), None, "sky"),
            P("ma", "freq", None, "pol", None),
            P("ma"),
            P("freq"),
            P("freq", "pol"),
        ),
        out_specs=(P(None, "freq", "ma", "pol", "sky"), P(("sky", "freq"))),
        check_vma=False,
    )
```

```python
import functools

import jax
import jax.numpy as jnp
from jax import lax
from jax.experimental import pallas as pl
from jax.experimental.pallas import tpu as pltpu
from jax.sharding import PartitionSpec as P

MESH = pl.DeviceIdType.MESH


def arrival_order(n, i):
    return sorted((j for j in range(n) if j != i), key=lambda j: (abs(j - i), j))


def send_order(n, i):
    order = sorted((j for j in range(n) if j != i), key=lambda j: (abs(j - i), (j > i) != (2 * i < n)))
    return order[:1] + order[:0:-1] if i in (0, n - 1) else order


def others(n, me, rule):
    if n > 8:
        ups = [jnp.where(me + s < n, me + s, n - 1 - s) for s in range(1, n)]
        return ups
    table = [rule(n, i) for i in range(n)]
    order = []
    for k in range(n - 1):
        pick = jnp.int32(table[0][k])
        for i in range(1, n):
            pick = jnp.where(me == i, jnp.int32(table[i][k]), pick)
        order.append(pick)
    return order


def step_kernel(
    sizes, total, alm_ref, beam_ref, m_ref, mask_ref, noise_ref, out_ref, power_ref,
    recv, wide, acc, beam_v, inv_n, rs_n, mine, slots,
    z_send, z_recv, p_send, p_recv, own_sem, beam_sem, q_send, q_recv, chain, meet,
):
    n_ma, n_freq, n_pol = sizes
    n_all = n_ma * n_freq * n_pol
    ma, freq, pol = lax.axis_index("ma"), lax.axis_index("freq"), lax.axis_index("pol")
    block, columns = alm_ref.shape[2], alm_ref.shape[3]
    groups, _, rows, _ = recv.shape
    per_source = n_pol * block
    per_group = rows // per_source
    modes = beam_ref.shape[1]
    my_slot = (freq * n_ma + ma) * n_pol + pol

    def place(slot):
        return {"ma": lax.rem(slot // n_pol, n_ma), "freq": slot // (n_pol * n_ma), "pol": lax.rem(slot, n_pol)}

    def for_peers(body):
        if n_all <= 32:
            for r in range(1, n_all):
                body(r)
        else:
            lax.fori_loop(1, n_all, lambda r, _: (body(r), 0)[1], 0)

    beam_copy = pltpu.make_async_copy(beam_ref, beam_v, beam_sem)
    beam_copy.start()

    barrier = pltpu.get_barrier_semaphore()

    def tell_line(sem):
        @pl.when(ma > 0)
        def _():
            pl.semaphore_signal(sem, inc=1, device_id={"ma": ma - 1}, device_id_type=MESH)

        @pl.when(ma < n_ma - 1)
        def _():
            pl.semaphore_signal(sem, inc=1, device_id={"ma": ma + 1}, device_id_type=MESH)

    def tell(axis, me, n, sem):
        for q in range(1, n):
            pl.semaphore_signal(sem, inc=1, device_id={axis: lax.rem(me + q, n)}, device_id_type=MESH)

    beside = jnp.where(ma > 0, 1, 0) + jnp.where(ma < n_ma - 1, 1, 0)
    tell_line(barrier)
    tell("pol", pol, n_pol, barrier)
    tell("freq", freq, n_freq, barrier)

    def part(source, core, c):
        start = lax.rem(source, per_group) * per_source + core * block
        return recv.at[source // per_group, c, pl.ds(pl.multiple_of(start, block), block)]

    own = [pltpu.make_async_copy(alm_ref.at[ma, c], part(ma, pol, c), own_sem.at[c]) for c in range(2)]
    for copy in own:
        copy.start()
    pl.semaphore_wait(barrier, beside + n_pol - 1 + n_freq - 1)

    order = others(n_ma, ma, arrival_order)
    targets = others(n_ma, ma, send_order)
    sends = []

    def send(k):
        for c in range(2):
            sends.append(pltpu.make_async_remote_copy(
                src_ref=alm_ref.at[targets[k], c], dst_ref=part(ma, pol, c),
                send_sem=z_send.at[k, c], recv_sem=z_recv.at[ma, c],
                device_id={"ma": targets[k]}, device_id_type=MESH))
            sends[-1].start()

    if n_ma <= 8:
        send(0)
    for t in range(n_ma - 2):
        tell_line(chain.at[t])
        pl.semaphore_wait(chain.at[t], beside)
    for k in range(len(sends) // 2, n_ma - 1):
        send(k)

    def relay(source, c, src):
        hops = []
        for q in range(1, n_pol):
            hops.append(pltpu.make_async_remote_copy(
                src_ref=src, dst_ref=part(source, pol, c),
                send_sem=p_send.at[source, c], recv_sem=p_recv.at[source, c],
                device_id={"pol": lax.rem(pol + q, n_pol)}, device_id_type=MESH))
            hops[-1].start()
        return hops

    def arrival(source, c):
        return pltpu.make_async_remote_copy(
            src_ref=alm_ref.at[source, c], dst_ref=part(source, pol, c),
            send_sem=z_send.at[0, c], recv_sem=z_recv.at[source, c],
            device_id={"ma": source}, device_id_type=MESH)

    relays = [relay(ma, c, alm_ref.at[ma, c]) for c in range(2)]

    spread = jnp.transpose(jnp.broadcast_to(noise_ref[...], (128, modes)))
    inv_n[...] = 1.0 / spread
    rs_n[...] = lax.rsqrt(spread)
    mine[1:2, :] = jnp.full((1, 128), mask_ref[0].astype(jnp.float32))
    beam_copy.wait()
    strip = min(modes, 128)

    def widen(i, _):
        k0 = pl.multiple_of(i * strip, strip)
        for g in range(groups):
            degree = lax.broadcasted_iota(jnp.int32, (strip, rows), 1) + g * rows
            keep = degree >= m_ref[0]
            zero = jnp.zeros((strip, rows), jnp.float32)
            b0 = jnp.where(keep, beam_v[0, pl.ds(k0, strip), g * rows:(g + 1) * rows].astype(jnp.float32), zero)
            b1 = jnp.where(keep, beam_v[1, pl.ds(k0, strip), g * rows:(g + 1) * rows].astype(jnp.float32), zero)
            wide[g, 0, pl.ds(k0, strip), :] = b0.astype(wide.dtype)
            wide[g, 1, pl.ds(k0, strip), :] = (-b1).astype(wide.dtype)
            wide[g, 0, pl.ds(modes + k0, strip), :] = b1.astype(wide.dtype)
            wide[g, 1, pl.ds(modes + k0, strip), :] = b0.astype(wide.dtype)
        return 0

    lax.fori_loop(0, modes // strip, widen, 0)
    tell("pol", pol, n_pol, meet.at[0])
    pl.semaphore_wait(meet.at[0], n_pol - 1)
    tell("freq", freq, n_freq, meet.at[1])
    pl.semaphore_wait(meet.at[1], n_freq - 1)

    tile = min(modes, 256)
    tiles = 2 * modes // tile

    def accumulate(g, first):
        def body(i, _):
            k0 = pl.multiple_of(i * tile, tile)
            value = jnp.dot(wide[g, 0, pl.ds(k0, tile), :], recv[g, 0], preferred_element_type=jnp.float32)
            value += jnp.dot(wide[g, 1, pl.ds(k0, tile), :], recv[g, 1], preferred_element_type=jnp.float32)
            acc[pl.ds(k0, tile), :] = value if first else acc[pl.ds(k0, tile), :] + value
            return 0
        lax.fori_loop(0, tiles, body, 0)

    def squares(value, k0):
        noise_rows = inv_n[k0 % modes:k0 % modes + tile, :]
        sums = jnp.zeros((tile, 128), jnp.float32)
        for j in range(columns // 128):
            part_j = value[:, j * 128:(j + 1) * 128]
            sums += part_j * part_j
        return jnp.sum(sums * noise_rows, axis=0, keepdims=True)

    def finish(steps):
        power = jnp.zeros((1, 128), jnp.float32)
        for i in range(tiles):
            k0 = i * tile
            value = acc[k0:k0 + tile, :]
            for g, c in steps:
                value += jnp.dot(wide[g, c, k0:k0 + tile, :], recv[g, c], preferred_element_type=jnp.float32)
            acc[k0:k0 + tile, :] = value
            power += squares(value, k0)
        return power

    def add_half(g, c):
        for i in range(tiles):
            k0 = i * tile
            acc[k0:k0 + tile, :] += jnp.dot(wide[g, c, k0:k0 + tile, :], recv[g, c], preferred_element_type=jnp.float32)

    for copy in own:
        copy.wait()
    for c in range(2):
        for hop in relays[c]:
            hop.wait()
    if per_group == 1:
        accumulate(ma, True)
        for k, source in enumerate(order):
            later = []
            for c in range(2):
                arrival(source, c).wait_recv()
                later.append(relay(source, c, part(source, pol, c)))
            if k < len(order) - 1:
                for c in range(2):
                    for hop in later[c]:
                        hop.wait()
                accumulate(source, False)
            else:
                for hop in later[0]:
                    hop.wait()
                add_half(source, 0)
                for hop in later[1]:
                    hop.wait()
                power = finish([(source, 1)])
    else:
        later = []
        for source in order:
            for c in range(2):
                arrival(source, c).wait_recv()
                later.append(relay(source, c, part(source, pol, c)))
        for hops in later:
            for hop in hops:
                hop.wait()
        for g in range(groups):
            accumulate(g, g == 0)
        power = finish([])

    mine[0:1, :] = power
    slots[my_slot, 0:1, :] = power
    slots[my_slot, 1:2, :] = mine[1:2, :]

    def report(r):
        return pltpu.make_async_remote_copy(
            src_ref=mine, dst_ref=slots.at[my_slot], send_sem=q_send.at[r - 1], recv_sem=q_recv.at[my_slot],
            device_id=place(lax.rem(my_slot + r, n_all)), device_id_type=MESH)

    def heard(r):
        source = lax.rem(my_slot + r, n_all)
        pltpu.make_async_remote_copy(
            src_ref=mine, dst_ref=slots.at[source], send_sem=q_send.at[r - 1], recv_sem=q_recv.at[source],
            device_id=place(source), device_id_type=MESH).wait_recv()

    for_peers(lambda r: report(r).start())
    for copy in sends:
        copy.wait_send()
    for_peers(heard)

    per_freq = n_ma * n_pol
    masked, live, here = 0.0, 0.0, 0.0
    for f in range(n_freq):
        channel = jnp.sum(jnp.sum(slots[f * per_freq:(f + 1) * per_freq, 0, :], axis=0, keepdims=True), axis=1, keepdims=True) / total
        flag = slots[f * per_freq, 1:2, 0:1]
        masked += flag * channel
        live += flag
        here += jnp.where(freq == f, channel, 0.0)
    band = masked / live
    factor = mine[1:2, 0:1] / jnp.sqrt(0.5 * here + 0.5 * band + 1e-06)
    power_ref[0] = here[0, 0]

    def rescale(i, _):
        k0 = pl.multiple_of(i * strip, strip)
        scale = rs_n[pl.ds(k0, strip), :] * factor
        for c in range(2):
            for j in range(columns // 128):
                value = acc[pl.ds(c * modes + k0, strip), j * 128:(j + 1) * 128]
                out_ref[c, pl.ds(k0, strip), j * 128:(j + 1) * 128] = (value * scale).astype(out_ref.dtype)
        return 0

    lax.fori_loop(0, modes // strip, rescale, 0)
    for_peers(lambda r: report(r).wait_send())


def on_device(sizes, alm, beam, m_table, chan_mask, noise):
    n_ma, n_freq, n_pol = sizes
    planes = jnp.transpose(alm[:, 0], (2, 0, 1, 3))
    response = beam[0, 0]
    block, columns = planes.shape[2], planes.shape[3]
    modes, degrees = response.shape[1], response.shape[2]
    per_source = n_pol * block
    rows = per_source * max(1, min(n_ma, 256 // per_source))
    groups = degrees // rows
    n_all = n_ma * n_freq * n_pol
    total = float(n_ma * modes * n_pol * columns)
    vmem = pl.BlockSpec(memory_space=pltpu.VMEM)
    smem = pl.BlockSpec(memory_space=pltpu.SMEM)
    dma = pltpu.SemaphoreType.DMA
    scaled, power = pl.pallas_call(
        functools.partial(step_kernel, sizes, total),
        out_shape=(
            jax.ShapeDtypeStruct((2, modes, columns), jnp.bfloat16),
            jax.ShapeDtypeStruct((1,), jnp.float32),
        ),
        in_specs=[vmem, pl.BlockSpec(memory_space=pl.ANY), smem, smem, vmem],
        out_specs=(vmem, smem),
        scratch_shapes=[
            pltpu.VMEM((groups, 2, rows, columns), jnp.bfloat16),
            pltpu.VMEM((groups, 2, 2 * modes, rows), jnp.bfloat16),
            pltpu.VMEM((2 * modes, columns), jnp.float32),
            pltpu.VMEM((2, modes, degrees), jnp.bfloat16),
            pltpu.VMEM((modes, 128), jnp.float32),
            pltpu.VMEM((modes, 128), jnp.float32),
            pltpu.VMEM((2, 128), jnp.float32),
            pltpu.VMEM((n_all, 2, 128), jnp.float32),
            dma((n_ma, 2)), dma((n_ma, 2)), dma((n_ma, 2)), dma((n_ma, 2)), dma((2,)), dma,
            dma((n_all,)), dma((n_all,)),
            pltpu.SemaphoreType.REGULAR((max(1, n_ma - 2),)), pltpu.SemaphoreType.REGULAR((2,)),
        ],
        compiler_params=pltpu.CompilerParams(collective_id=0, has_side_effects=True, vmem_limit_bytes=40 * 1024 * 1024),
        name="driftscan_step",
    )(planes, response, m_table, chan_mask, noise)
    return scaled[:, None, None], power


def solution(mesh):
    sizes = (mesh.shape["ma"], mesh.shape["freq"], mesh.shape["pol"])
    return jax.shard_map(
        functools.partial(on_device, sizes),
        mesh=mesh,
        in_specs=(
            P(None, "freq", ("ma", "pol"), None, "sky"),
            P("ma", "freq", None, "pol", None),
            P("ma"),
            P("freq"),
            P("freq", "pol"),
        ),
        out_specs=(P(None, "freq", "ma", "pol", "sky"), P(("sky", "freq"))),
        check_vma=False,
    )
```

```python
import functools

import jax
import jax.numpy as jnp
from jax import lax
from jax.experimental import pallas as pl
from jax.experimental.pallas import tpu as pltpu
from jax.sharding import PartitionSpec as P

MESH = pl.DeviceIdType.MESH


def arrival_order(n, i):
    return sorted((j for j in range(n) if j != i), key=lambda j: (abs(j - i), j))


def send_order(n, i):
    order = sorted((j for j in range(n) if j != i), key=lambda j: (abs(j - i), (j > i) != (2 * i < n)))
    return order[:1] + order[:0:-1] if i in (0, n - 1) else order


def others(n, me, rule):
    if n > 8:
        ups = [jnp.where(me + s < n, me + s, n - 1 - s) for s in range(1, n)]
        return ups
    table = [rule(n, i) for i in range(n)]
    order = []
    for k in range(n - 1):
        pick = jnp.int32(table[0][k])
        for i in range(1, n):
            pick = jnp.where(me == i, jnp.int32(table[i][k]), pick)
        order.append(pick)
    return order


def step_kernel(
    sizes, total, alm_ref, beam_ref, m_hbm, mask_hbm, noise_hbm, acc, scale_ref, power_ref,
    recv, wide, beam_v, inv_n, rs_n, mine, slots, m_ref, mask_ref, noise_ref,
    z_send, z_recv, p_send, p_recv, own_sem, beam_sem, q_send, q_recv, chain, meet, small_sem,
):
    n_ma, n_freq, n_pol = sizes
    n_all = n_ma * n_freq * n_pol
    ma, freq, pol = lax.axis_index("ma"), lax.axis_index("freq"), lax.axis_index("pol")
    block, columns = alm_ref.shape[2], alm_ref.shape[3]
    groups, _, rows, _ = recv.shape
    per_source = n_pol * block
    per_group = rows // per_source
    modes = beam_ref.shape[1]
    my_slot = (freq * n_ma + ma) * n_pol + pol

    def place(slot):
        return {"ma": lax.rem(slot // n_pol, n_ma), "freq": slot // (n_pol * n_ma), "pol": lax.rem(slot, n_pol)}

    def for_peers(body):
        if n_all <= 32:
            for r in range(1, n_all):
                body(r)
        else:
            lax.fori_loop(1, n_all, lambda r, _: (body(r), 0)[1], 0)

    beam_copy = pltpu.make_async_copy(beam_ref, beam_v, beam_sem)
    beam_copy.start()
    small = [
        pltpu.make_async_copy(src, dst, small_sem.at[i])
        for i, (src, dst) in enumerate(((m_hbm, m_ref), (mask_hbm, mask_ref), (noise_hbm, noise_ref)))
    ]
    for copy in small:
        copy.start()

    barrier = pltpu.get_barrier_semaphore()

    def tell_line(sem):
        @pl.when(ma > 0)
        def _():
            pl.semaphore_signal(sem, inc=1, device_id={"ma": ma - 1}, device_id_type=MESH)

        @pl.when(ma < n_ma - 1)
        def _():
            pl.semaphore_signal(sem, inc=1, device_id={"ma": ma + 1}, device_id_type=MESH)

    def tell(axis, me, n, sem):
        for q in range(1, n):
            pl.semaphore_signal(sem, inc=1, device_id={axis: lax.rem(me + q, n)}, device_id_type=MESH)

    beside = jnp.where(ma > 0, 1, 0) + jnp.where(ma < n_ma - 1, 1, 0)
    tell_line(barrier)
    tell("pol", pol, n_pol, barrier)
    tell("freq", freq, n_freq, barrier)

    def part(source, core, c):
        start = lax.rem(source, per_group) * per_source + core * block
        return recv.at[source // per_group, c, pl.ds(pl.multiple_of(start, block), block)]

    own = [pltpu.make_async_copy(alm_ref.at[ma, c], part(ma, pol, c), own_sem.at[c]) for c in range(2)]
    for copy in own:
        copy.start()
    pl.semaphore_wait(barrier, beside + n_pol - 1 + n_freq - 1)

    order = others(n_ma, ma, arrival_order)
    targets = others(n_ma, ma, send_order)
    sends = []

    def send(k):
        for c in range(2):
            sends.append(pltpu.make_async_remote_copy(
                src_ref=alm_ref.at[targets[k], c], dst_ref=part(ma, pol, c),
                send_sem=z_send.at[k, c], recv_sem=z_recv.at[ma, c],
                device_id={"ma": targets[k]}, device_id_type=MESH))
            sends[-1].start()

    if n_ma <= 8:
        send(0)
    for t in range(n_ma - 2):
        tell_line(chain.at[t])
        pl.semaphore_wait(chain.at[t], beside)
    for k in range(len(sends) // 2, n_ma - 1):
        send(k)

    def relay(source, c, src):
        hops = []
        for q in range(1, n_pol):
            hops.append(pltpu.make_async_remote_copy(
                src_ref=src, dst_ref=part(source, pol, c),
                send_sem=p_send.at[source, c], recv_sem=p_recv.at[source, c],
                device_id={"pol": lax.rem(pol + q, n_pol)}, device_id_type=MESH))
            hops[-1].start()
        return hops

    def arrival(source, c):
        return pltpu.make_async_remote_copy(
            src_ref=alm_ref.at[source, c], dst_ref=part(source, pol, c),
            send_sem=z_send.at[0, c], recv_sem=z_recv.at[source, c],
            device_id={"ma": source}, device_id_type=MESH)

    relays = [relay(ma, c, alm_ref.at[ma, c]) for c in range(2)]

    for copy in small:
        copy.wait()
    spread = jnp.transpose(jnp.broadcast_to(noise_ref[...], (128, modes)))
    inv_n[...] = 1.0 / spread
    rs_n[...] = lax.rsqrt(spread)
    mine[1:2, :] = jnp.full((1, 128), mask_ref[0].astype(jnp.float32))
    beam_copy.wait()
    strip = min(modes, 128)

    def widen(i, _):
        k0 = pl.multiple_of(i * strip, strip)
        for g in range(groups):
            degree = lax.broadcasted_iota(jnp.int32, (strip, rows), 1) + g * rows
            keep = degree >= m_ref[0]
            zero = jnp.zeros((strip, rows), jnp.float32)
            b0 = jnp.where(keep, beam_v[0, pl.ds(k0, strip), g * rows:(g + 1) * rows].astype(jnp.float32), zero)
            b1 = jnp.where(keep, beam_v[1, pl.ds(k0, strip), g * rows:(g + 1) * rows].astype(jnp.float32), zero)
            wide[g, 0, pl.ds(k0, strip), :] = b0.astype(wide.dtype)
            wide[g, 1, pl.ds(k0, strip), :] = (-b1).astype(wide.dtype)
            wide[g, 0, pl.ds(modes + k0, strip), :] = b1.astype(wide.dtype)
            wide[g, 1, pl.ds(modes + k0, strip), :] = b0.astype(wide.dtype)
        return 0

    lax.fori_loop(0, modes // strip, widen, 0)
    tell("pol", pol, n_pol, meet.at[0])
    pl.semaphore_wait(meet.at[0], n_pol - 1)
    tell("freq", freq, n_freq, meet.at[1])
    pl.semaphore_wait(meet.at[1], n_freq - 1)

    tile = min(modes, 256)
    tiles = 2 * modes // tile

    def accumulate(g, first):
        def body(i, _):
            k0 = pl.multiple_of(i * tile, tile)
            value = jnp.dot(wide[g, 0, pl.ds(k0, tile), :], recv[g, 0], preferred_element_type=jnp.float32)
            value += jnp.dot(wide[g, 1, pl.ds(k0, tile), :], recv[g, 1], preferred_element_type=jnp.float32)
            acc[pl.ds(k0, tile), :] = value if first else acc[pl.ds(k0, tile), :] + value
            return 0
        lax.fori_loop(0, tiles, body, 0)

    def squares(value, k0):
        noise_rows = inv_n[k0 % modes:k0 % modes + tile, :]
        sums = jnp.zeros((tile, 128), jnp.float32)
        for j in range(columns // 128):
            part_j = value[:, j * 128:(j + 1) * 128]
            sums += part_j * part_j
        return jnp.sum(sums * noise_rows, axis=0, keepdims=True)

    def finish(steps):
        power = jnp.zeros((1, 128), jnp.float32)
        for i in range(tiles):
            k0 = i * tile
            value = acc[k0:k0 + tile, :]
            for g, c in steps:
                value += jnp.dot(wide[g, c, k0:k0 + tile, :], recv[g, c], preferred_element_type=jnp.float32)
            acc[k0:k0 + tile, :] = value
            power += squares(value, k0)
        return power

    def add_half(g, c):
        for i in range(tiles):
            k0 = i * tile
            acc[k0:k0 + tile, :] += jnp.dot(wide[g, c, k0:k0 + tile, :], recv[g, c], preferred_element_type=jnp.float32)

    for copy in own:
        copy.wait()
    for c in range(2):
        for hop in relays[c]:
            hop.wait()
    if per_group == 1:
        accumulate(ma, True)
        for k, source in enumerate(order):
            later = []
            for c in range(2):
                arrival(source, c).wait_recv()
                later.append(relay(source, c, part(source, pol, c)))
            if k < len(order) - 1:
                for c in range(2):
                    for hop in later[c]:
                        hop.wait()
                accumulate(source, False)
            else:
                for hop in later[0]:
                    hop.wait()
                add_half(source, 0)
                for hop in later[1]:
                    hop.wait()
                power = finish([(source, 1)])
    else:
        later = []
        for source in order:
            for c in range(2):
                arrival(source, c).wait_recv()
                later.append(relay(source, c, part(source, pol, c)))
        for hops in later:
            for hop in hops:
                hop.wait()
        for g in range(groups):
            accumulate(g, g == 0)
        power = finish([])

    mine[0:1, :] = power
    slots[my_slot, 0:1, :] = power
    slots[my_slot, 1:2, :] = mine[1:2, :]

    def report(r):
        return pltpu.make_async_remote_copy(
            src_ref=mine, dst_ref=slots.at[my_slot], send_sem=q_send.at[r - 1], recv_sem=q_recv.at[my_slot],
            device_id=place(lax.rem(my_slot + r, n_all)), device_id_type=MESH)

    def heard(r):
        source = lax.rem(my_slot + r, n_all)
        pltpu.make_async_remote_copy(
            src_ref=mine, dst_ref=slots.at[source], send_sem=q_send.at[r - 1], recv_sem=q_recv.at[source],
            device_id=place(source), device_id_type=MESH).wait_recv()

    for_peers(lambda r: report(r).start())
    for copy in sends:
        copy.wait_send()
    for_peers(heard)

    per_freq = n_ma * n_pol
    masked, live, here = 0.0, 0.0, 0.0
    for f in range(n_freq):
        channel = jnp.sum(jnp.sum(slots[f * per_freq:(f + 1) * per_freq, 0, :], axis=0, keepdims=True), axis=1, keepdims=True) / total
        flag = slots[f * per_freq, 1:2, 0:1]
        masked += flag * channel
        live += flag
        here += jnp.where(freq == f, channel, 0.0)
    band = masked / live
    factor = mine[1:2, 0:1] / jnp.sqrt(0.5 * here + 0.5 * band + 1e-06)
    power_ref[...] = jnp.broadcast_to(here, power_ref.shape)
    scale_ref[...] = rs_n[...] * factor
    for_peers(lambda r: report(r).wait_send())


def rescale_kernel(acc, scale_ref, power_ref, out_ref, channel_ref, staged, sems):
    modes = scale_ref.shape[0]
    columns = acc.shape[1]
    strip = modes // sems.shape[0]
    channel_ref[0] = power_ref[0, 0]
    copies = []
    for i in range(sems.shape[0]):
        k0 = i * strip
        scale = scale_ref[k0:k0 + strip, :]
        for c in range(2):
            for j in range(columns // 128):
                value = acc[c * modes + k0:c * modes + k0 + strip, j * 128:(j + 1) * 128]
                staged[c, k0:k0 + strip, j * 128:(j + 1) * 128] = (value * scale).astype(staged.dtype)
        copies.append(pltpu.make_async_copy(
            staged.at[:, pl.ds(k0, strip)], out_ref.at[:, pl.ds(k0, strip)], sems.at[i]))
        copies[-1].start()
    for copy in copies:
        copy.wait()


def on_device(sizes, alm, beam, m_table, chan_mask, noise):
    n_ma, n_freq, n_pol = sizes
    planes = jnp.transpose(alm[:, 0], (2, 0, 1, 3))
    response = beam[0, 0]
    block, columns = planes.shape[2], planes.shape[3]
    modes, degrees = response.shape[1], response.shape[2]
    per_source = n_pol * block
    rows = per_source * max(1, min(n_ma, 256 // per_source))
    groups = degrees // rows
    n_all = n_ma * n_freq * n_pol
    total = float(n_ma * modes * n_pol * columns)
    vmem = pl.BlockSpec(memory_space=pltpu.VMEM)
    smem = pl.BlockSpec(memory_space=pltpu.SMEM)
    dma = pltpu.SemaphoreType.DMA
    hbm = pl.BlockSpec(memory_space=pl.ANY)
    visibility, scale, power = pl.pallas_call(
        functools.partial(step_kernel, sizes, total),
        out_shape=(
            jax.ShapeDtypeStruct((2 * modes, columns), jnp.float32),
            jax.ShapeDtypeStruct((modes, 128), jnp.float32),
            jax.ShapeDtypeStruct((1, 128), jnp.float32),
        ),
        in_specs=[vmem, hbm, hbm, hbm, hbm],
        out_specs=(vmem, vmem, vmem),
        scratch_shapes=[
            pltpu.VMEM((groups, 2, rows, columns), jnp.bfloat16),
            pltpu.VMEM((groups, 2, 2 * modes, rows), jnp.bfloat16),
            pltpu.VMEM((2, modes, degrees), jnp.bfloat16),
            pltpu.VMEM((modes, 128), jnp.float32),
            pltpu.VMEM((modes, 128), jnp.float32),
            pltpu.VMEM((2, 128), jnp.float32),
            pltpu.VMEM((n_all, 2, 128), jnp.float32),
            pltpu.SMEM((1,), jnp.int32),
            pltpu.SMEM((1,), jnp.int32),
            pltpu.VMEM((1, modes), jnp.float32),
            dma((n_ma, 2)), dma((n_ma, 2)), dma((n_ma, 2)), dma((n_ma, 2)), dma((2,)), dma,
            dma((n_all,)), dma((n_all,)),
            pltpu.SemaphoreType.REGULAR((max(1, n_ma - 2),)), pltpu.SemaphoreType.REGULAR((2,)), dma((3,)),
        ],
        compiler_params=pltpu.CompilerParams(collective_id=0, has_side_effects=True, vmem_limit_bytes=40 * 1024 * 1024),
        name="driftscan_step",
    )(planes, response, m_table, chan_mask, noise)
    pieces = 4 if modes % 64 == 0 else 1
    scaled, channel_power = pl.pallas_call(
        rescale_kernel,
        out_shape=(
            jax.ShapeDtypeStruct((2, modes, columns), jnp.bfloat16),
            jax.ShapeDtypeStruct((1,), jnp.float32),
        ),
        in_specs=[vmem, vmem, vmem],
        out_specs=(hbm, smem),
        scratch_shapes=[pltpu.VMEM((2, modes, columns), jnp.bfloat16), dma((pieces,))],
        compiler_params=pltpu.CompilerParams(vmem_limit_bytes=16 * 1024 * 1024),
        name="rescale",
    )(visibility, scale, power)
    return scaled[:, None, None], channel_power


def solution(mesh):
    sizes = (mesh.shape["ma"], mesh.shape["freq"], mesh.shape["pol"])
    return jax.shard_map(
        functools.partial(on_device, sizes),
        mesh=mesh,
        in_specs=(
            P(None, "freq", ("ma", "pol"), None, "sky"),
            P("ma", "freq", None, "pol", None),
            P("ma"),
            P("freq"),
            P("freq", "pol"),
        ),
        out_specs=(P(None, "freq", "ma", "pol", "sky"), P(("sky", "freq"))),
        check_vma=False,
    )
```

```python
import functools

import jax
import jax.numpy as jnp
from jax import lax
from jax.experimental import pallas as pl
from jax.experimental.pallas import tpu as pltpu
from jax.sharding import PartitionSpec as P

MESH = pl.DeviceIdType.MESH


def arrival_order(n, i):
    return sorted((j for j in range(n) if j != i), key=lambda j: (abs(j - i), j))


def send_order(n, i):
    order = sorted((j for j in range(n) if j != i), key=lambda j: (abs(j - i), (j > i) != (2 * i < n)))
    return order[:1] + order[:0:-1] if i in (0, n - 1) else order


def others(n, me, rule):
    if n > 8:
        ups = [jnp.where(me + s < n, me + s, n - 1 - s) for s in range(1, n)]
        return ups
    table = [rule(n, i) for i in range(n)]
    order = []
    for k in range(n - 1):
        pick = jnp.int32(table[0][k])
        for i in range(1, n):
            pick = jnp.where(me == i, jnp.int32(table[i][k]), pick)
        order.append(pick)
    return order


def step_kernel(
    sizes, total, alm_ref, beam_ref, m_hbm, mask_hbm, noise_hbm, acc, scale_ref, power_ref,
    recv, wide, beam_v, inv_n, rs_n, mine, slots, m_ref, mask_ref, noise_ref,
    z_send, z_recv, p_send, p_recv, own_sem, beam_sem, q_send, q_recv, chain, meet, small_sem,
):
    n_ma, n_freq, n_pol = sizes
    n_all = n_ma * n_freq * n_pol
    ma, freq, pol = lax.axis_index("ma"), lax.axis_index("freq"), lax.axis_index("pol")
    block, columns = alm_ref.shape[2], alm_ref.shape[3]
    groups, _, rows, _ = recv.shape
    per_source = n_pol * block
    per_group = rows // per_source
    modes = beam_ref.shape[1]
    my_slot = (freq * n_ma + ma) * n_pol + pol

    def place(slot):
        return {"ma": lax.rem(slot // n_pol, n_ma), "freq": slot // (n_pol * n_ma), "pol": lax.rem(slot, n_pol)}

    def for_peers(body):
        if n_all <= 32:
            for r in range(1, n_all):
                body(r)
        else:
            lax.fori_loop(1, n_all, lambda r, _: (body(r), 0)[1], 0)

    beam_copy = pltpu.make_async_copy(beam_ref, beam_v, beam_sem)
    beam_copy.start()
    small = [
        pltpu.make_async_copy(src, dst, small_sem.at[i])
        for i, (src, dst) in enumerate(((m_hbm, m_ref), (mask_hbm, mask_ref), (noise_hbm, noise_ref)))
    ]
    for copy in small:
        copy.start()

    barrier = pltpu.get_barrier_semaphore()

    def tell_line(sem):
        @pl.when(ma > 0)
        def _():
            pl.semaphore_signal(sem, inc=1, device_id={"ma": ma - 1}, device_id_type=MESH)

        @pl.when(ma < n_ma - 1)
        def _():
            pl.semaphore_signal(sem, inc=1, device_id={"ma": ma + 1}, device_id_type=MESH)

    def tell(axis, me, n, sem):
        for q in range(1, n):
            pl.semaphore_signal(sem, inc=1, device_id={axis: lax.rem(me + q, n)}, device_id_type=MESH)

    beside = jnp.where(ma > 0, 1, 0) + jnp.where(ma < n_ma - 1, 1, 0)
    tell_line(barrier)
    tell("pol", pol, n_pol, barrier)
    tell("freq", freq, n_freq, barrier)

    def part(source, core, c):
        start = lax.rem(source, per_group) * per_source + core * block
        return recv.at[source // per_group, c, pl.ds(pl.multiple_of(start, block), block)]

    own = [pltpu.make_async_copy(alm_ref.at[ma, c], part(ma, pol, c), own_sem.at[c]) for c in range(2)]
    for copy in own:
        copy.start()
    pl.semaphore_wait(barrier, beside + n_pol - 1 + n_freq - 1)

    order = others(n_ma, ma, arrival_order)
    targets = others(n_ma, ma, send_order)
    sends = []

    def send(k):
        for c in range(2):
            sends.append(pltpu.make_async_remote_copy(
                src_ref=alm_ref.at[targets[k], c], dst_ref=part(ma, pol, c),
                send_sem=z_send.at[k, c], recv_sem=z_recv.at[ma, c],
                device_id={"ma": targets[k]}, device_id_type=MESH))
            sends[-1].start()

    if n_ma <= 8:
        send(0)
    for t in range(n_ma - 2):
        tell_line(chain.at[t])
        pl.semaphore_wait(chain.at[t], beside)
    for k in range(len(sends) // 2, n_ma - 1):
        send(k)

    def relay(source, c, src):
        hops = []
        for q in range(1, n_pol):
            hops.append(pltpu.make_async_remote_copy(
                src_ref=src, dst_ref=part(source, pol, c),
                send_sem=p_send.at[source, c], recv_sem=p_recv.at[source, c],
                device_id={"pol": lax.rem(pol + q, n_pol)}, device_id_type=MESH))
            hops[-1].start()
        return hops

    def arrival(source, c):
        return pltpu.make_async_remote_copy(
            src_ref=alm_ref.at[source, c], dst_ref=part(source, pol, c),
            send_sem=z_send.at[0, c], recv_sem=z_recv.at[source, c],
            device_id={"ma": source}, device_id_type=MESH)

    relays = [relay(ma, c, alm_ref.at[ma, c]) for c in range(2)]

    for copy in small:
        copy.wait()
    spread = jnp.transpose(jnp.broadcast_to(noise_ref[...], (128, modes)))
    inv_n[...] = 1.0 / spread
    rs_n[...] = lax.rsqrt(spread)
    mine[1:2, :] = jnp.full((1, 128), mask_ref[0].astype(jnp.float32))
    beam_copy.wait()
    strip = min(modes, 128)

    def widen(i, _):
        k0 = pl.multiple_of(i * strip, strip)
        for g in range(groups):
            degree = lax.broadcasted_iota(jnp.int32, (strip, rows), 1) + g * rows
            keep = degree >= m_ref[0]
            zero = jnp.zeros((strip, rows), jnp.float32)
            b0 = jnp.where(keep, beam_v[0, pl.ds(k0, strip), g * rows:(g + 1) * rows].astype(jnp.float32), zero)
            b1 = jnp.where(keep, beam_v[1, pl.ds(k0, strip), g * rows:(g + 1) * rows].astype(jnp.float32), zero)
            wide[g, 0, pl.ds(k0, strip), :] = b0.astype(wide.dtype)
            wide[g, 1, pl.ds(k0, strip), :] = (-b1).astype(wide.dtype)
            wide[g, 0, pl.ds(modes + k0, strip), :] = b1.astype(wide.dtype)
            wide[g, 1, pl.ds(modes + k0, strip), :] = b0.astype(wide.dtype)
        return 0

    lax.fori_loop(0, modes // strip, widen, 0)
    tell("pol", pol, n_pol, meet.at[0])
    pl.semaphore_wait(meet.at[0], n_pol - 1)
    tell("freq", freq, n_freq, meet.at[1])
    pl.semaphore_wait(meet.at[1], n_freq - 1)

    tile = min(modes, 512)
    tiles = 2 * modes // tile

    def accumulate(g, first):
        def body(i, _):
            k0 = pl.multiple_of(i * tile, tile)
            value = jnp.dot(wide[g, 0, pl.ds(k0, tile), :], recv[g, 0], preferred_element_type=jnp.float32)
            value += jnp.dot(wide[g, 1, pl.ds(k0, tile), :], recv[g, 1], preferred_element_type=jnp.float32)
            acc[pl.ds(k0, tile), :] = value if first else acc[pl.ds(k0, tile), :] + value
            return 0
        lax.fori_loop(0, tiles, body, 0)

    def squares(value, k0):
        noise_rows = inv_n[k0 % modes:k0 % modes + tile, :]
        sums = jnp.zeros((tile, 128), jnp.float32)
        for j in range(columns // 128):
            part_j = value[:, j * 128:(j + 1) * 128]
            sums += part_j * part_j
        return jnp.sum(sums * noise_rows, axis=0, keepdims=True)

    def finish(steps):
        power = jnp.zeros((1, 128), jnp.float32)
        for i in range(tiles):
            k0 = i * tile
            value = acc[k0:k0 + tile, :]
            for g, c in steps:
                value += jnp.dot(wide[g, c, k0:k0 + tile, :], recv[g, c], preferred_element_type=jnp.float32)
            acc[k0:k0 + tile, :] = value
            power += squares(value, k0)
        return power

    def add_half(g, c):
        for i in range(tiles):
            k0 = i * tile
            acc[k0:k0 + tile, :] += jnp.dot(wide[g, c, k0:k0 + tile, :], recv[g, c], preferred_element_type=jnp.float32)

    for copy in own:
        copy.wait()
    for c in range(2):
        for hop in relays[c]:
            hop.wait()
    if per_group == 1:
        accumulate(ma, True)
        for k, source in enumerate(order):
            later = []
            for c in range(2):
                arrival(source, c).wait_recv()
                later.append(relay(source, c, part(source, pol, c)))
            if k < len(order) - 1:
                for c in range(2):
                    for hop in later[c]:
                        hop.wait()
                accumulate(source, False)
            else:
                for hop in later[0]:
                    hop.wait()
                add_half(source, 0)
                for hop in later[1]:
                    hop.wait()
                power = finish([(source, 1)])
    else:
        later = []
        for source in order:
            for c in range(2):
                arrival(source, c).wait_recv()
                later.append(relay(source, c, part(source, pol, c)))
        for hops in later:
            for hop in hops:
                hop.wait()
        for g in range(groups):
            accumulate(g, g == 0)
        power = finish([])

    mine[0:1, :] = power
    slots[my_slot, 0:1, :] = power
    slots[my_slot, 1:2, :] = mine[1:2, :]

    def report(r):
        return pltpu.make_async_remote_copy(
            src_ref=mine, dst_ref=slots.at[my_slot], send_sem=q_send.at[r - 1], recv_sem=q_recv.at[my_slot],
            device_id=place(lax.rem(my_slot + r, n_all)), device_id_type=MESH)

    def heard(r):
        source = lax.rem(my_slot + r, n_all)
        pltpu.make_async_remote_copy(
            src_ref=mine, dst_ref=slots.at[source], send_sem=q_send.at[r - 1], recv_sem=q_recv.at[source],
            device_id=place(source), device_id_type=MESH).wait_recv()

    for_peers(lambda r: report(r).start())
    for copy in sends:
        copy.wait_send()
    for_peers(heard)

    per_freq = n_ma * n_pol
    masked, live, here = 0.0, 0.0, 0.0
    for f in range(n_freq):
        channel = jnp.sum(jnp.sum(slots[f * per_freq:(f + 1) * per_freq, 0, :], axis=0, keepdims=True), axis=1, keepdims=True) / total
        flag = slots[f * per_freq, 1:2, 0:1]
        masked += flag * channel
        live += flag
        here += jnp.where(freq == f, channel, 0.0)
    band = masked / live
    factor = mine[1:2, 0:1] / jnp.sqrt(0.5 * here + 0.5 * band + 1e-06)
    power_ref[...] = jnp.broadcast_to(here, power_ref.shape)
    scale_ref[...] = rs_n[...] * factor
    for_peers(lambda r: report(r).wait_send())


def rescale_kernel(acc, scale_ref, power_ref, out_ref, channel_ref, staged, sems):
    modes = scale_ref.shape[0]
    columns = acc.shape[1]
    strip = modes // sems.shape[0]
    channel_ref[0] = power_ref[0, 0]
    copies = []
    for i in range(sems.shape[0]):
        k0 = i * strip
        scale = scale_ref[k0:k0 + strip, :]
        for c in range(2):
            for j in range(columns // 128):
                value = acc[c * modes + k0:c * modes + k0 + strip, j * 128:(j + 1) * 128]
                staged[c, k0:k0 + strip, j * 128:(j + 1) * 128] = (value * scale).astype(staged.dtype)
        copies.append(pltpu.make_async_copy(
            staged.at[:, pl.ds(k0, strip)], out_ref.at[:, pl.ds(k0, strip)], sems.at[i]))
        copies[-1].start()
    for copy in copies:
        copy.wait()


def on_device(sizes, alm, beam, m_table, chan_mask, noise):
    n_ma, n_freq, n_pol = sizes
    planes = jnp.transpose(alm[:, 0], (2, 0, 1, 3))
    response = beam[0, 0]
    block, columns = planes.shape[2], planes.shape[3]
    modes, degrees = response.shape[1], response.shape[2]
    per_source = n_pol * block
    rows = per_source * max(1, min(n_ma, 256 // per_source))
    groups = degrees // rows
    n_all = n_ma * n_freq * n_pol
    total = float(n_ma * modes * n_pol * columns)
    vmem = pl.BlockSpec(memory_space=pltpu.VMEM)
    smem = pl.BlockSpec(memory_space=pltpu.SMEM)
    dma = pltpu.SemaphoreType.DMA
    hbm = pl.BlockSpec(memory_space=pl.ANY)
    visibility, scale, power = pl.pallas_call(
        functools.partial(step_kernel, sizes, total),
        out_shape=(
            jax.ShapeDtypeStruct((2 * modes, columns), jnp.float32),
            jax.ShapeDtypeStruct((modes, 128), jnp.float32),
            jax.ShapeDtypeStruct((1, 128), jnp.float32),
        ),
        in_specs=[vmem, hbm, hbm, hbm, hbm],
        out_specs=(vmem, vmem, vmem),
        scratch_shapes=[
            pltpu.VMEM((groups, 2, rows, columns), jnp.bfloat16),
            pltpu.VMEM((groups, 2, 2 * modes, rows), jnp.bfloat16),
            pltpu.VMEM((2, modes, degrees), jnp.bfloat16),
            pltpu.VMEM((modes, 128), jnp.float32),
            pltpu.VMEM((modes, 128), jnp.float32),
            pltpu.VMEM((2, 128), jnp.float32),
            pltpu.VMEM((n_all, 2, 128), jnp.float32),
            pltpu.SMEM((1,), jnp.int32),
            pltpu.SMEM((1,), jnp.int32),
            pltpu.VMEM((1, modes), jnp.float32),
            dma((n_ma, 2)), dma((n_ma, 2)), dma((n_ma, 2)), dma((n_ma, 2)), dma((2,)), dma,
            dma((n_all,)), dma((n_all,)),
            pltpu.SemaphoreType.REGULAR((max(1, n_ma - 2),)), pltpu.SemaphoreType.REGULAR((2,)), dma((3,)),
        ],
        compiler_params=pltpu.CompilerParams(collective_id=0, has_side_effects=True, vmem_limit_bytes=40 * 1024 * 1024),
        name="driftscan_step",
    )(planes, response, m_table, chan_mask, noise)
    pieces = 4 if modes % 64 == 0 else 1
    scaled, channel_power = pl.pallas_call(
        rescale_kernel,
        out_shape=(
            jax.ShapeDtypeStruct((2, modes, columns), jnp.bfloat16),
            jax.ShapeDtypeStruct((1,), jnp.float32),
        ),
        in_specs=[vmem, vmem, vmem],
        out_specs=(hbm, smem),
        scratch_shapes=[pltpu.VMEM((2, modes, columns), jnp.bfloat16), dma((pieces,))],
        compiler_params=pltpu.CompilerParams(vmem_limit_bytes=16 * 1024 * 1024),
        name="rescale",
    )(visibility, scale, power)
    return scaled[:, None, None], channel_power


def solution(mesh):
    sizes = (mesh.shape["ma"], mesh.shape["freq"], mesh.shape["pol"])
    return jax.shard_map(
        functools.partial(on_device, sizes),
        mesh=mesh,
        in_specs=(
            P(None, "freq", ("ma", "pol"), None, "sky"),
            P("ma", "freq", None, "pol", None),
            P("ma"),
            P("freq"),
            P("freq", "pol"),
        ),
        out_specs=(P(None, "freq", "ma", "pol", "sky"), P(("sky", "freq"))),
        check_vma=False,
    )
```
